32 devices in a mesh: section: 2 (over core), dp: 4 (over z), tensor: 4 (over y, x).
Axes of the slice: x: 2, y: 2, z: 4, core: 2. Of those that a mesh axis runs over, the one named last changes fastest.
Arguments:
- inputs: bfloat16 [2, 4, 1024, 768], P(None, 'dp', 'tensor'), may hold values from -6 to 6
- segment_ids: int32 [2, 4, 1024], P(None, 'dp'), may hold values from 0 to 7, never falling along the last dimension, each value on 1 to 384 neighbouring positions
- cotangent: float32 [2, 4, 1024, 768], P(None, 'dp', 'tensor'), may hold values from -6 to 6
- qkv_weight: bfloat16 [2, 3, 768, 768], P('section', None, 'dp', 'tensor'), may hold values from -0.21875 to 0.21875
- out_weight: bfloat16 [2, 768, 768], P('section', 'tensor', 'dp'), may hold values from -0.875 to 0.875
- up_weight: bfloat16 [2, 768, 3072], P('section', 'dp', 'tensor'), may hold values from -0.21875 to 0.21875
- down_weight: bfloat16 [2, 3072, 768], P('section', 'tensor', 'dp'), may hold values from -0.109375 to 0.109375
- norm_gain: float32 [2, 2, 768], P('section'), may hold values from 0.5 to 1.5
- norm_bias: float32 [2, 2, 768], P('section'), may hold values from -4 to 4
- qv_bias: float32 [2, 2, 768], P('section'), may hold values from -6 to 6
- up_bias: float32 [2, 3072], P('section'), may hold values from -6 to 6
- resid_bias: float32 [2, 768], P('section'), may hold values from -6 to 6
Outputs:
- outputs: float32 [2, 2, 4, 1024, 768], P('section', None, 'dp', 'tensor')
- input_grads: float32 [2, 2, 4, 1024, 768], P('section', None, 'dp', 'tensor')
- qkv_grad: float32 [2, 3, 768, 768], P('section', None, 'dp', 'tensor')
- out_grad: float32 [2, 768, 768], P('section', 'tensor', 'dp')
- up_grad: float32 [2, 768, 3072], P('section', 'dp', 'tensor')
- down_grad: float32 [2, 3072, 768], P('section', 'tensor', 'dp')
- gain_grad: float32 [2, 2, 768], P('section')
- norm_bias_grad: float32 [2, 2, 768], P('section')
- qv_bias_grad: float32 [2, 2, 768], P('section')
- up_bias_grad: float32 [2, 3072], P('section')
- resid_bias_grad: float32 [2, 768], P('section')
The draws below stay inside these ranges and needn't reach their ends.
Inputs may be any that keep to these rules, and one draw needn't show every extreme that they name: `segment_ids`: along each sequence the ids never fall; every id 0 to 7 holds 1 to 384 tokens, one of them exactly 384.
All inputs are finite; a program needn't handle non-finite values.
Results may differ from the reference program's by a relative error of at most 0.012.
Values may be sent and summed in bfloat16 or wider, within the bound.
A program may use at most 256 MiB of HBM per device.

```python
import math
import jax
import jax.numpy as jnp
import numpy as np
from jax import lax

D = 768
HEADS = 12
HEAD_DIM = 64
ROT = 16
FF = 3072
MICRO = 2
L = 1024
SEGMENTS = 8
HDIM = 768
SEQS = 4
SEG_MOST = 384


def with_spikes(array, rng, source, target, blocks, factor):
    owner, partner = [(jnp.arange(array.shape[position]) // (array.shape[position] // blocks)).reshape([-1 if axis == position else 1 for axis in range(array.ndim)]) for position in (source, target)]
    chosen = jax.random.permutation(rng, blocks)[partner]
    strong = (owner == chosen) | (owner == (partner + blocks // 2) % blocks)
    return jnp.where(strong, factor * array, array)


def level_of(rng, extent, split, low, largest):
    def one(dim, blocks):
        steps = jax.random.uniform(jax.random.fold_in(jax.random.fold_in(rng, 6), dim), (blocks,), jnp.float32, low / len(split), largest / len(split))
        return jnp.repeat(jnp.exp(steps), extent[dim] // blocks).reshape((-1,) + (1,) * (len(extent) - dim - 1))

    gain = one(*split[0])
    for cut in split[1:]:
        gain = gain * one(*cut)
    return gain


def profile(number_of, total, bound, slope):
    weights = [(1 << 20) // math.isqrt(standing ** slope) + 1 for standing in range(2, number_of + 1)]
    rest, given = total - bound - (number_of - 1), [1] * (number_of - 1)
    while rest > 0:
        movable = [i for i in range(number_of - 1) if given[i] < bound]
        mass, remaining = sum([weights[i] for i in movable]), rest
        for i in movable:
            more = min(bound - given[i], max(1, remaining * weights[i] // mass), rest)
            given[i] = given[i] + more
            rest = rest - more
    return np.array([bound] + given)


def uneven(key, number_of, total, bound, skew):
    if number_of == 2:
        one = jax.random.randint(key, (), max(1, total - bound), min(bound, total - 1) + 1)
        return jnp.stack([one, total - one])
    sizes = jnp.asarray(profile(number_of, total, bound, skew), jnp.int32)
    couples = (number_of - 1) // 2
    giver, taker = sizes[1:1 + 2 * couples:2], sizes[2:2 + 2 * couples:2]
    room = jnp.minimum(giver - 1, bound - taker)
    passed = jax.random.randint(jax.random.fold_in(key, 1), (couples,), 0, 1 << 20) % (room + 1)
    sizes = sizes.at[1:1 + 2 * couples:2].set(giver - passed).at[2:2 + 2 * couples:2].set(taker + passed)
    return sizes[jax.random.permutation(jax.random.fold_in(key, 2), number_of)]


def bell_draw(key, extent, spread, bound, split=(), kind=jnp.bfloat16):
    array = jax.random.normal(key, extent, jnp.float32) * spread
    if len(split) > 0:
        array = level_of(key, extent, split, -0.22, 0.18) * array
    return jnp.clip(array, min=-bound, max=bound).astype(kind)


def bell_draw_with(own_key, dims, spread, most, split, heavy, dtype=jnp.bfloat16):
    values = spread * jax.random.normal(own_key, dims, jnp.float32)
    if split:
        values = values * level_of(own_key, dims, split, -0.22, 0.18)
    return jnp.clip(with_spikes(values, jax.random.fold_in(own_key, 3), *heavy), -most, most).astype(dtype)


def setup_inputs(seed: int = 0) -> dict:
    splits = jax.random.split(jax.random.key(seed), 13)
    inputs = bell_draw(splits[0], (MICRO, SEQS, L, D), 1.0, 6.0, ((1, 4), (2, 4)))
    segment_ids = jax.vmap(lambda own: jnp.searchsorted(jnp.cumsum(uneven(own, SEGMENTS, L, SEG_MOST, 1)), jnp.arange(L), side="right"))(jax.random.split(splits[1], MICRO * SEQS)).reshape((MICRO, SEQS, L)).astype(jnp.int32)
    cotangent = bell_draw_with(splits[2], (MICRO, SEQS, L, D), 1.0, 6.0, ((1, 4), (2, 4)), (1, 3, 4, 2.0), jnp.float32)
    qkv_weight = bell_draw(splits[3], (2, 3, D, HDIM), D ** -0.5, 0.21875, ((0, 2), (2, 4), (3, 4)))
    out_weight = bell_draw(splits[4], (2, HDIM, D), (HDIM // 16) ** -0.5, 0.875, ((0, 2), (1, 4), (2, 4)))
    up_weight = bell_draw(splits[5], (2, D, FF), D ** -0.5, 0.21875, ((0, 2), (1, 4), (2, 4)))
    down_weight = bell_draw(splits[6], (2, FF, D), FF ** -0.5, 0.109375, ((0, 2), (1, 4), (2, 4)))
    norm_gain = jnp.clip(1.0 + 0.1 * jax.random.normal(splits[7], (2, 2, D), jnp.float32), 0.5, 1.5)
    norm_bias = bell_draw(splits[8], (2, 2, D), 0.3, 4.0, ((0, 2),), jnp.float32)
    qv_bias = bell_draw(splits[9], (2, 2, HDIM), 0.5, 6.0, ((0, 2),), jnp.float32)
    up_bias = bell_draw(splits[10], (2, FF), 0.5, 6.0, ((0, 2),), jnp.float32)
    resid_bias = bell_draw(splits[11], (2, D), 0.5, 6.0, ((0, 2),), jnp.float32)
    return {"inputs": inputs, "segment_ids": segment_ids, "cotangent": cotangent, "qkv_weight": qkv_weight, "out_weight": out_weight, "up_weight": up_weight, "down_weight": down_weight, "norm_gain": norm_gain, "norm_bias": norm_bias, "qv_bias": qv_bias, "up_bias": up_bias, "resid_bias": resid_bias}


epsilon = 1e-05
root_half = 0.7071067811865476
inv_root_tau = 0.3989422804014327
masked_score = -1e+30

def normalize(values, gain_row, shift_row):
    centre = lax.optimization_barrier(jnp.mean(values, axis=-1, keepdims=True))
    centred = values - centre
    inverse = lax.rsqrt(lax.optimization_barrier(jnp.mean(centred * centred, axis=-1, keepdims=True)) + epsilon)
    unit_rows = centred * inverse
    return (unit_rows, inverse, unit_rows * gain_row + shift_row)

def normalize_back(incoming, unit_rows, inverse, gain_row):
    scaled = incoming * gain_row
    return inverse * (scaled - lax.optimization_barrier(jnp.mean(scaled, axis=-1, keepdims=True)) - unit_rows * lax.optimization_barrier(jnp.mean(scaled * unit_rows, axis=-1, keepdims=True)))

def gelu_value(values):
    return values * 0.5 * (1.0 + lax.erf(values * root_half))

def gelu_slope(values):
    return 0.5 * (1.0 + lax.erf(values * root_half)) + values * inv_root_tau * jnp.exp(-0.5 * values * values)

def rotary_tables(length, rotated):
    positions = lax.broadcasted_iota(jnp.float32, (length, rotated // 2), 0)
    orders = lax.broadcasted_iota(jnp.float32, (length, rotated // 2), 1)
    angles = positions * jnp.exp(orders * (-2.0 * math.log(10000.0) / rotated))
    return (jnp.cos(angles), jnp.sin(angles))

def rotate(head_vals, cosine_table, sine_table, direction):
    half_rot = cosine_table.shape[-1]
    lower_part = head_vals[..., :half_rot]
    upper_part = head_vals[..., half_rot:2 * half_rot]
    turned = direction * sine_table
    return jnp.concatenate([lower_part * cosine_table - upper_part * turned, upper_part * cosine_table + lower_part * turned, head_vals[..., 2 * half_rot:]], axis=-1)

def as_float(values):
    return values.astype(jnp.float32)

def layer_forward(row_in, segments, layer, cosine_table, sine_table):
    query_key_value_matrix, output_matrix, up_matrix, down_matrix, gain_pair, shift_pair, qv_pair, up_bias_row, resid_row = layer
    length = row_in.shape[0]
    widened = row_in.astype(jnp.float32)
    unit_one, inverse_one, normed_one = normalize(widened, gain_pair[0], shift_pair[0])
    unit_two, inverse_two, normed_two = normalize(widened, gain_pair[1], shift_pair[1])
    attention_input = normed_one.astype(jnp.bfloat16)
    feedforward_input = normed_two.astype(jnp.bfloat16)
    projected_rows = jnp.einsum('ld,cde->cle', as_float(attention_input), as_float(query_key_value_matrix))
    cos_b = cosine_table[:, None, :]
    sin_b = sine_table[:, None, :]
    head_shape = (length, HEADS, HEAD_DIM)
    query_b = (rotate((projected_rows[0] + qv_pair[0]).reshape(head_shape), cos_b, sin_b, 1.0) * 0.125).astype(jnp.bfloat16)
    key_b = rotate(projected_rows[1].reshape(head_shape), cos_b, sin_b, 1.0).astype(jnp.bfloat16)
    value_b = (projected_rows[2] + qv_pair[1]).reshape(head_shape).astype(jnp.bfloat16)
    positions = lax.broadcasted_iota(jnp.int32, (length, length), 0)
    key_pos = lax.broadcasted_iota(jnp.int32, (length, length), 1)
    allowed = (segments[:, None] == segments[None, :]) & (key_pos <= positions)
    scores = jnp.einsum('qhd,khd->hqk', as_float(query_b), as_float(key_b))
    scores = jnp.where(allowed[None], scores, masked_score)
    row_top = lax.optimization_barrier(jnp.max(scores, axis=-1, keepdims=True))
    log_total = row_top + jnp.log(lax.optimization_barrier(jnp.sum(jnp.exp(scores - row_top), axis=-1, keepdims=True)))
    probs = jnp.exp(scores - log_total)
    probs_b = probs.astype(jnp.bfloat16)
    context = jnp.einsum('hqk,khd->qhd', as_float(probs_b), as_float(value_b)).astype(jnp.bfloat16)
    flattened_context = context.reshape(length, HDIM)
    up_pre = jnp.dot(feedforward_input, up_matrix, preferred_element_type=jnp.float32) + up_bias_row
    hidden_block = gelu_value(up_pre).astype(jnp.bfloat16)
    branch = jnp.dot(flattened_context, output_matrix, preferred_element_type=jnp.float32) + jnp.dot(hidden_block, down_matrix, preferred_element_type=jnp.float32)
    result = widened + branch + resid_row
    saved = (unit_one, inverse_one, unit_two, inverse_two, attention_input, feedforward_input, query_b, key_b, value_b, probs, probs_b, flattened_context, up_pre, hidden_block)
    return (result, saved)

def layer_backward(row_in, segments, incoming, layer, cosine_table, sine_table):
    query_key_value_matrix, output_matrix, up_matrix, down_matrix, gain_pair, shift_pair, qv_pair, up_bias_row, resid_row = layer
    result, saved = layer_forward(row_in, segments, layer, cosine_table, sine_table)
    unit_one, inverse_one, unit_two, inverse_two, attention_input, feedforward_input, query_b, key_b, value_b, probs, probs_b, flattened_context, up_pre, hidden_block = saved
    length = row_in.shape[0]
    grad_b = incoming.astype(jnp.bfloat16)
    down_weight_gradient = jnp.dot(hidden_block.T, grad_b, preferred_element_type=jnp.float32)
    output_weight_gradient = jnp.dot(flattened_context.T, grad_b, preferred_element_type=jnp.float32)
    resid_g = lax.optimization_barrier(jnp.sum(incoming, axis=0))
    pre_grad = jnp.dot(grad_b, down_matrix.T, preferred_element_type=jnp.float32) * gelu_slope(up_pre)
    up_bias_g = lax.optimization_barrier(jnp.sum(pre_grad, axis=0))
    preactivation_block = pre_grad.astype(jnp.bfloat16)
    up_weight_gradient = jnp.dot(feedforward_input.T, preactivation_block, preferred_element_type=jnp.float32)
    feedforward_input_gradient = jnp.dot(preactivation_block, up_matrix.T, preferred_element_type=jnp.float32)
    context_gradient = jnp.dot(grad_b, output_matrix.T, preferred_element_type=jnp.float32).astype(jnp.bfloat16)
    context_gradient = context_gradient.reshape(length, HEADS, HEAD_DIM)
    value_grad = jnp.einsum('hqk,qhd->khd', as_float(probs_b), as_float(context_gradient))
    prob_grad = jnp.einsum('qhd,khd->hqk', as_float(context_gradient), as_float(value_b))
    score_grad = probs * (prob_grad - lax.optimization_barrier(jnp.sum(probs * prob_grad, axis=-1, keepdims=True)))
    score_b = score_grad.astype(jnp.bfloat16)
    query_grad = jnp.einsum('hqk,khd->qhd', as_float(score_b), as_float(key_b))
    key_grad = jnp.einsum('hqk,qhd->khd', as_float(score_b), as_float(query_b))
    cos_b = cosine_table[:, None, :]
    sin_b = sine_table[:, None, :]
    query_grad = rotate(query_grad, cos_b, sin_b, -1.0) * 0.125
    key_grad = rotate(key_grad, cos_b, sin_b, -1.0)
    stacked = jnp.stack([query_grad.reshape(length, HDIM), key_grad.reshape(length, HDIM), value_grad.reshape(length, HDIM)])
    qv_g = jnp.stack([lax.optimization_barrier(jnp.sum(stacked[0], axis=0)), lax.optimization_barrier(jnp.sum(stacked[2], axis=0))])
    stacked_block = stacked.astype(jnp.bfloat16)
    query_key_value_gradient = jnp.einsum('ld,cle->cde', as_float(attention_input), as_float(stacked_block))
    attn_in_grad = jnp.einsum('cle,cde->ld', as_float(stacked_block), as_float(query_key_value_matrix))
    gain_g = jnp.stack([lax.optimization_barrier(jnp.sum(attn_in_grad * unit_one, axis=0)), lax.optimization_barrier(jnp.sum(feedforward_input_gradient * unit_two, axis=0))])
    shift_g = jnp.stack([lax.optimization_barrier(jnp.sum(attn_in_grad, axis=0)), lax.optimization_barrier(jnp.sum(feedforward_input_gradient, axis=0))])
    input_grad = incoming + normalize_back(attn_in_grad, unit_one, inverse_one, gain_pair[0]) + normalize_back(feedforward_input_gradient, unit_two, inverse_two, gain_pair[1])
    return (input_grad, (query_key_value_gradient, output_weight_gradient, up_weight_gradient, down_weight_gradient, gain_g, shift_g, qv_g, up_bias_g, resid_g))

def reference(inputs, segment_ids, cotangent, qkv_weight, out_weight, up_weight, down_weight, norm_gain, norm_bias, qv_bias, up_bias, resid_bias):
    cosine_table, sine_table = rotary_tables(L, ROT)
    flat_in = inputs.reshape(-1, L, D)
    flat_segs = segment_ids.reshape(-1, L)
    flat_cot = cotangent.reshape(-1, L, D)

    def layer_of(number):
        return (qkv_weight[number], out_weight[number], up_weight[number], down_weight[number], norm_gain[number], norm_bias[number], qv_bias[number], up_bias[number], resid_bias[number])

    def run_layer(layer, row_sets):

        def one_seq(pair):
            made, saved = layer_forward(pair[0], pair[1], layer, cosine_table, sine_table)
            return made
        return lax.map(one_seq, (row_sets, flat_segs))

    def back_layer(layer, row_sets, grad_sets):
        zeros_tree = (jnp.zeros(layer[0].shape, jnp.float32), jnp.zeros(layer[1].shape, jnp.float32), jnp.zeros(layer[2].shape, jnp.float32), jnp.zeros(layer[3].shape, jnp.float32), jnp.zeros(layer[4].shape, jnp.float32), jnp.zeros(layer[5].shape, jnp.float32), jnp.zeros(layer[6].shape, jnp.float32), jnp.zeros(layer[7].shape, jnp.float32), jnp.zeros(layer[8].shape, jnp.float32))

        def step_fn(running, item):
            input_grad, parts = layer_backward(item[0], item[1], item[2], layer, cosine_table, sine_table)
            return (jax.tree.map(lambda left, right: left + right, running, parts), input_grad)
        return lax.scan(step_fn, zeros_tree, (row_sets, flat_segs, grad_sets))
    layer_zero = layer_of(0)
    layer_one = layer_of(1)
    wide_one = run_layer(layer_zero, flat_in)
    hidden_one = wide_one.astype(jnp.bfloat16)
    wide_two = run_layer(layer_one, hidden_one)
    totals_one, grad_mid = back_layer(layer_one, hidden_one, flat_cot)
    totals_zero, grad_first = back_layer(layer_zero, flat_in, grad_mid)
    out_shape = inputs.shape
    outputs = jnp.stack([wide_one.reshape(out_shape), wide_two.reshape(out_shape)])
    input_grads = jnp.stack([grad_first.reshape(out_shape), grad_mid.reshape(out_shape)])
    stacked = [jnp.stack([totals_zero[number], totals_one[number]]) for number in range(9)]
    return (outputs, input_grads, stacked[0], stacked[1], stacked[2], stacked[3], stacked[4], stacked[5], stacked[6], stacked[7], stacked[8])
```

```python
import functools
import math

import jax
import jax.numpy as jnp
from jax import lax
from jax.experimental import pallas as pl
from jax.experimental.pallas import tpu as pltpu
from jax.sharding import PartitionSpec as P

HEAD_DIM = 64
ROT = 16
DOC_MOST = 384
QB = 256
EPS = 1e-05
ROOT_HALF = 0.7071067811865476
INV_ROOT_TAU = 0.3989422804014327
MASKED = -1e30
LANES = 128
SEC, DP, TEN = "section", "dp", "tensor"

F32 = jnp.float32
BF16 = jnp.bfloat16
MESH = pl.DeviceIdType.MESH
ANY = pl.ANY
VMEM_LIMIT = 62 * 1024 * 1024


def dot(a, b):
    return lax.dot_general(a, b, (((1,), (0,)), ((), ())), preferred_element_type=F32)


def dot_bt(a, b):
    return lax.dot_general(a, b, (((1,), (1,)), ((), ())), preferred_element_type=F32)


def dot_at(a, b):
    return lax.dot_general(a, b, (((0,), (0,)), ((), ())), preferred_element_type=F32)


def rows_of(index, size):
    return pl.ds(pl.multiple_of(index * size, size), size)


class Dims:
    def __init__(self, mesh_shape, inputs, segments, qkv, up):
        self.n_s = mesh_shape[SEC]
        self.n_z = mesh_shape[DP]
        self.n_t = mesh_shape[TEN]
        self.R = inputs[2]
        self.D = inputs[3]
        self.T = segments[2]
        self.HC = qkv[3]
        self.HP = -(-self.HC // 256) * 256
        self.NH = self.HC // HEAD_DIM
        self.FF = up[2]
        self.DW = qkv[2]
        self.NQ = self.T // QB
        self.k0 = [max(0, QB * (j + 1) - QB - DOC_MOST) for j in range(self.NQ)]
        self.kw = [QB * (j + 1) - self.k0[j] for j in range(self.NQ)]
        self.off = [sum(self.kw[:j]) for j in range(self.NQ)]
        self.KR = sum(self.kw)
        self.KM = max(self.kw)
        self.starts = [0, self.HP, 2 * self.HP]


class Place:
    def __init__(self, dm):
        self.s = lax.axis_index(SEC)
        self.z = lax.axis_index(DP)
        self.t = lax.axis_index(TEN)
        self.dm = dm

    def tensor_peer(self, k):
        return lax.rem(self.t + k, self.dm.n_t)

    def tensor_source(self, k):
        return lax.rem(self.t + self.dm.n_t - k, self.dm.n_t)

    def dp_peer(self, k):
        return lax.rem(self.z + k, self.dm.n_z)

    def dp_source(self, k):
        return lax.rem(self.z + self.dm.n_z - k, self.dm.n_z)

    def greet(self, dp):
        barrier = pltpu.get_barrier_semaphore()
        count = 0
        for k in range(1, self.dm.n_t):
            pl.semaphore_signal(
                barrier, inc=1, device_id={TEN: self.tensor_peer(k)}, device_id_type=MESH
            )
            count += 1
        if dp:
            for k in range(1, self.dm.n_z):
                pl.semaphore_signal(
                    barrier, inc=1, device_id={DP: self.dp_peer(k)}, device_id_type=MESH
                )
                count += 1
        pl.semaphore_signal(barrier, inc=1, device_id={SEC: 1 - self.s}, device_id_type=MESH)
        count += 1
        pl.semaphore_wait(barrier, count)


def remote(src, dst, send_sem, recv_sem, axis, peer):
    return pltpu.make_async_remote_copy(
        src_ref=src,
        dst_ref=dst,
        send_sem=send_sem,
        recv_sem=recv_sem,
        device_id={axis: peer},
        device_id_type=MESH,
    )


def unit_rows(values):
    centre = jnp.mean(values, axis=-1, keepdims=True)
    centred = values - centre
    inverse = lax.rsqrt(jnp.mean(centred * centred, axis=-1, keepdims=True) + EPS)
    return centred * inverse, inverse


def partner_lanes(values):
    width = values.shape[1]
    lane = lax.broadcasted_iota(jnp.int32, values.shape, 1) & (HEAD_DIM - 1)
    up = pltpu.roll(values, width - ROT // 2, 1)
    down = pltpu.roll(values, ROT // 2, 1)
    return jnp.where(lane < ROT // 2, up, down)


def norm_rows(dm, x_ref, a_ref, m_ref, n_ref, gain, shift, b):
    rows = rows_of(b, dm.R)
    unit, _ = unit_rows(x_ref[rows, :].astype(F32))
    n_ref[rows, :] = unit.astype(BF16)
    a_ref[rows, :] = (unit * gain[0:1, :] + shift[0:1, :]).astype(BF16)
    m_ref[rows, :] = (unit * gain[1:2, :] + shift[1:2, :]).astype(BF16)


def widen(dm, table):
    return jnp.concatenate([table] * (dm.HP // LANES), axis=1)


def rotary_tables(dm, ct_ref, st_ref):
    lane = lax.broadcasted_iota(jnp.int32, (QB, LANES), 1) & (HEAD_DIM - 1)
    order = (lane & (ROT // 2 - 1)).astype(F32)
    step = jnp.exp(order * (-2.0 * math.log(10000.0) / ROT))

    def body(b, carry):
        place = (lax.broadcasted_iota(jnp.int32, (QB, LANES), 0) + b * QB).astype(F32)
        angle = place * step
        sine = jnp.sin(angle)
        rows = rows_of(b, QB)
        ct_ref[rows, :] = jnp.where(lane < ROT, jnp.cos(angle), 1.0)
        st_ref[rows, :] = jnp.where(lane < ROT // 2, -sine, jnp.where(lane < ROT, sine, 0.0))
        return carry

    lax.fori_loop(0, dm.T // QB, body, 0)


def mask_bias(dm, seg_row, bias_ref):
    for j in range(dm.NQ):
        q0, k0, kw, off = QB * j, dm.k0[j], dm.kw[j], dm.off[j]
        query_seg = seg_row[:, q0 : q0 + QB]
        for i in range(kw // LANES):
            start = k0 + i * LANES
            key_seg = jnp.broadcast_to(seg_row[:, start : start + LANES], (QB, LANES)).T
            key = lax.broadcasted_iota(jnp.int32, (LANES, QB), 0) + start
            query = lax.broadcasted_iota(jnp.int32, (LANES, QB), 1) + q0
            allowed = (key_seg == query_seg) & (key <= query)
            bias_ref[off + i * LANES : off + (i + 1) * LANES, :] = jnp.where(allowed, 0.0, MASKED)


def project_rows(dm, a_ref, wqkv_ref, qvb, ct_ref, st_ref, q_ref, k_ref, v_ref, qt_ref, kt_ref, vt_ref, b):
    HP = dm.HP
    rows = rows_of(b, QB)
    acc = dot(a_ref[rows, :], wqkv_ref[...])
    ct, st = widen(dm, ct_ref[rows, :]), widen(dm, st_ref[rows, :])
    q = acc[:, 0:HP] + qvb[0:1, :]
    q = ((q * ct + partner_lanes(q) * st) * 0.125).astype(BF16)
    k = acc[:, HP : 2 * HP]
    k = (k * ct + partner_lanes(k) * st).astype(BF16)
    v = (acc[:, 2 * HP : 3 * HP] + qvb[1:2, :]).astype(BF16)
    q_ref[rows, :] = q
    k_ref[rows, :] = k
    v_ref[rows, :] = v
    qt_ref[:, rows] = q.T
    kt_ref[:, rows] = k.T
    vt_ref[:, rows] = v.T


def attend(dm, k_ref, qt_ref, qtm, vt_ref, bias_ref, pt_ref, ct_ref, c_ref):
    HP = dm.HP
    row = lax.broadcasted_iota(jnp.int32, (HP, QB), 0)
    ct_ref[...] = jnp.zeros_like(ct_ref)
    for j in range(dm.NQ):
        q0, k0, kw, off = QB * j, dm.k0[j], dm.kw[j], dm.off[j]
        for h in range(dm.NH):
            inside = (row >= h * HEAD_DIM) & (row < (h + 1) * HEAD_DIM)
            qtm[h] = jnp.where(inside, qt_ref[:, q0 : q0 + QB], jnp.zeros((HP, QB), BF16))

        def head(h, carry):
            hrows = rows_of(h, HEAD_DIM)
            scores = dot(k_ref[k0 : k0 + kw, :], qtm[h])
            scores = scores + bias_ref[off : off + kw, :]
            top = jnp.max(scores, axis=0, keepdims=True)
            probs = jnp.exp(scores - top)
            total = jnp.sum(probs, axis=0, keepdims=True)
            probs = (probs * (1.0 / total)).astype(BF16)
            pt_ref[off : off + kw, pl.ds(pl.multiple_of(h * QB, QB), QB)] = probs
            ct_ref[hrows, q0 : q0 + QB] = dot(vt_ref[hrows, k0 : k0 + kw], probs)
            return carry

        lax.fori_loop(0, dm.NH, head, 0)
        c_ref[q0 : q0 + QB, :] = ct_ref[:, q0 : q0 + QB].T.astype(BF16)


def hidden_rows(dm, m_ref, wup_ref, upb, h_ref, slope_ref, b):
    rows = rows_of(b, QB)
    u = dot(m_ref[rows, :], wup_ref[...]) + upb[...]
    cumulative = 0.5 * (1.0 + lax.erf(u * ROOT_HALF))
    h_ref[rows, :] = (u * cumulative).astype(BF16)
    slope_ref[rows, :] = (cumulative + u * INV_ROOT_TAU * jnp.exp(-0.5 * u * u)).astype(BF16)


def branch_rows(dm, c_ref, h_ref, wot_ref, wdt_ref, b):
    rows = rows_of(b, dm.R)
    return dot_bt(c_ref[rows, :], wot_ref[...]) + dot_bt(h_ref[rows, :], wdt_ref[...])


def pad_qkv(dm, raw_ref, out_ref):
    out_ref[...] = jnp.zeros_like(out_ref)
    for c in range(3):
        out_ref[:, c * dm.HP : c * dm.HP + dm.HC] = raw_ref[c]


def pad_heads(dm, raw_ref, out_ref):
    out_ref[...] = jnp.zeros_like(out_ref)
    out_ref[:, 0 : dm.HC] = raw_ref[...]


def small_width(dm):
    return max(dm.D, dm.FF, dm.HP)


def unpack_small(dm, ref):
    return (
        ref[0:2, 0 : dm.D],
        ref[2:4, 0 : dm.D],
        ref[6:8, 0 : dm.HP],
        ref[4:5, 0 : dm.FF],
        ref[5:6, 0 : dm.D],
    )


def pack_small(dm, t, gain, shift, qv, up, resid, out_ref):
    out_ref[...] = jnp.zeros_like(out_ref)
    out_ref[0:2, 0 : dm.D] = gain[...]
    out_ref[2:4, 0 : dm.D] = shift[...]
    out_ref[4:5, 0 : dm.FF] = up[:, pl.ds(pl.multiple_of(t * dm.FF, dm.FF), dm.FF)]
    out_ref[5:6, 0 : dm.D] = resid[...]
    for i in range(dm.n_t):

        @pl.when(t == i)
        def _(i=i):
            out_ref[6:8, 0 : dm.HC] = qv[:, i * dm.HC : (i + 1) * dm.HC]


def turn_shard(dm, wide, src, dst):
    rows, cols = src.shape
    whole_rows, whole_cols = -(-rows // QB) * QB, -(-cols // LANES) * LANES
    wide[0:whole_rows, 0:whole_cols] = jnp.zeros((whole_rows, whole_cols), wide.dtype)
    wide[0:rows, 0:cols] = src[...]
    for i in range(0, whole_rows, QB):
        n = min(QB, rows - i)
        dst[:, i : i + n] = wide[i : i + QB, 0:whole_cols].T[0:cols, 0:n]


def small_rows(dm):
    return (2, 8, small_width(dm))


def back_heads(dm, at, gb_ref, wot_ref, dc_ref, dct_ref):
    def body(b, carry):
        rows = rows_of(b, QB)
        grad = dot(gb_ref[rows, :], wot_ref[...]).astype(BF16)
        dc_ref[rows, :] = grad
        dct_ref[:, rows] = grad.T
        return carry

    lax.fori_loop(0, dm.T // QB, body, 0)


def attend_back(dm, q_ref, v_ref, kt_ref, pt_ref, dc_ref, dct_ref, qm, dcm, dctm, ds, dk_ref, dv_ref, dqt_ref):
    HP = dm.HP
    lane = lax.broadcasted_iota(jnp.int32, (QB, HP), 1)
    row = lax.broadcasted_iota(jnp.int32, (HP, QB), 0)
    dk_ref[...] = jnp.zeros_like(dk_ref)
    dv_ref[...] = jnp.zeros_like(dv_ref)
    dqt_ref[...] = jnp.zeros_like(dqt_ref)
    for j in range(dm.NQ):
        q0, k0, kw, off = QB * j, dm.k0[j], dm.kw[j], dm.off[j]
        for h in range(dm.NH):
            low, high = h * HEAD_DIM, (h + 1) * HEAD_DIM
            in_lane = (lane >= low) & (lane < high)
            in_row = (row >= low) & (row < high)
            zero = jnp.zeros((QB, HP), BF16)
            qm[h * QB : (h + 1) * QB, :] = jnp.where(in_lane, q_ref[q0 : q0 + QB, :], zero)
            dcm[h * QB : (h + 1) * QB, :] = jnp.where(in_lane, dc_ref[q0 : q0 + QB, :], zero)
            dctm[h] = jnp.where(in_row, dct_ref[:, q0 : q0 + QB], jnp.zeros((HP, QB), BF16))

        def head(h, carry):
            hrows = rows_of(h, HEAD_DIM)
            lanes = pl.ds(pl.multiple_of(h * QB, QB), QB)
            probs = pt_ref[off : off + kw, lanes].astype(F32)
            prob_grad = dot(v_ref[k0 : k0 + kw, :], dctm[h])
            mean = jnp.sum(probs * prob_grad, axis=0, keepdims=True)
            score = (probs * (prob_grad - mean)).astype(BF16)
            ds[0:kw, lanes] = score
            dqt_ref[hrows, q0 : q0 + QB] = dot(kt_ref[hrows, k0 : k0 + kw], score)
            return carry

        lax.fori_loop(0, dm.NH, head, 0)
        dv_ref[k0 : k0 + kw, :] += dot(pt_ref[off : off + kw, :], dcm[...])
        dk_ref[k0 : k0 + kw, :] += dot(ds[0:kw, :], qm[...])


def back_hidden(dm, r, gb_ref, acc):
    def body(b, carry):
        rows = rows_of(b, QB)
        du = dot(gb_ref[rows, :], r.wdt[...]) * r.slope[rows, :].astype(F32)
        acc[4:5, 0 : dm.FF] += jnp.sum(du, axis=0, keepdims=True)
        r.du[rows, :] = du.astype(BF16)
        return carry

    lax.fori_loop(0, dm.T // QB, body, 0)


def back_rows(dm, r, gain, acc, b):
    HP = dm.HP
    rows = rows_of(b, QB)
    unit = r.n[rows, :].astype(F32)
    dmid = dot_bt(r.du[rows, :], r.wup[...])
    acc[1:2, 0 : dm.D] += jnp.sum(dmid * unit, axis=0, keepdims=True)
    acc[3:4, 0 : dm.D] += jnp.sum(dmid, axis=0, keepdims=True)
    ct, st = widen(dm, r.ctab[rows, :]), widen(dm, r.stab[rows, :])
    dq = r.turned[:, rows].T
    dq = (dq * ct - partner_lanes(dq) * st) * 0.125
    acc[6:7, 0:HP] += jnp.sum(dq, axis=0, keepdims=True)
    r.dqkv[rows, 0:HP] = dq.astype(BF16)
    dk = r.dk[rows, :]
    r.dqkv[rows, HP : 2 * HP] = (dk * ct - partner_lanes(dk) * st).astype(BF16)
    dv = r.dv[rows, :]
    acc[7:8, 0:HP] += jnp.sum(dv, axis=0, keepdims=True)
    r.dqkv[rows, 2 * HP : 3 * HP] = dv.astype(BF16)
    datt = dot_bt(r.dqkv[rows, :], r.wqkv[...])
    acc[0:1, 0 : dm.D] += jnp.sum(datt * unit, axis=0, keepdims=True)
    acc[2:3, 0 : dm.D] += jnp.sum(datt, axis=0, keepdims=True)
    return datt * gain[0:1, :] + dmid * gain[1:2, :]


def weight_grad(dm, r, piece, gb_ref):
    def body(i, carry):
        cols = rows_of(i, QB)
        if piece == 0:
            made = dot_at(r.a[:, cols], r.dqkv[...])
            for c in range(3):
                r.wg[0][c, cols, :] = made[:, c * dm.HP : c * dm.HP + dm.HC].astype(BF16)
        elif piece == 1:
            r.wg[1][cols, :] = dot_at(r.m[:, cols], r.du[...]).astype(BF16)
        elif piece == 2:
            r.wg[2][cols, :] = dot_at(gb_ref[:, cols], r.c[...])[:, 0 : dm.HC].astype(BF16)
        else:
            r.wg[3][cols, :] = dot_at(gb_ref[:, cols], r.h[...]).astype(BF16)
        return carry

    lax.fori_loop(0, dm.D // QB, body, 0)


def norm_back(grad, values):
    unit, inverse = unit_rows(values)
    return inverse * (
        grad
        - jnp.mean(grad, axis=-1, keepdims=True)
        - unit * jnp.mean(grad * unit, axis=-1, keepdims=True)
    )


class Refs:
    pass


PIECES = range(4)
X0, GB1, Y0, X1, Y1, E1, GB0, E0, TS = CHANNELS = range(9)


def held_shapes(dm):
    T, D, HP, FF = dm.T, dm.D, dm.HP, dm.FF
    return dict(
        a=(T, D), m=(T, D), n=(T, D), h=(T, FF), slope=(T, FF), c=(T, HP), q=(T, HP), v=(T, HP), kt=(HP, T),
        pt=(dm.KR, dm.NH * QB), wqkv=(D, 3 * HP), wup=(D, FF), wot=(D, HP), wdt=(D, FF),
    )


def whole_shapes(dm):
    return [(3, dm.D, dm.HC), (dm.D, dm.FF), (dm.D, dm.HC), (dm.D, dm.FF)]


def part_shapes(dm):
    return [(3, dm.DW, dm.HC), (dm.DW, dm.FF), (dm.DW, dm.HC), (dm.DW, dm.FF)]


def out_layout(dm):
    S = jax.ShapeDtypeStruct
    block = S((dm.n_s, dm.R, dm.D), F32)
    return dict(
        o_y=block,
        o_g=block,
        o_w=[S(shape, F32) for shape in part_shapes(dm)],
        o_small=S((dm.n_t, 8, small_width(dm)), F32),
        land=[S(shape, BF16) for shape in whole_shapes(dm)],
        kept={name: S(shape, BF16) for name, shape in held_shapes(dm).items()},
    )


def scratch_layout(dm):
    T, D, R, HP, FF, HC, DW = dm.T, dm.D, dm.R, dm.HP, dm.FF, dm.HC, dm.DW
    NH, KR, KM, n_t, n_z = dm.NH, dm.KR, dm.KM, dm.n_t, dm.n_z
    W = small_width(dm)
    V, dma = pltpu.VMEM, pltpu.SemaphoreType.DMA
    raw, part = whole_shapes(dm), part_shapes(dm)
    rows = V((8, W), F32)
    peers = V((n_t - 1, R, D), BF16)
    layout = {name: V(shape, BF16) for name, shape in held_shapes(dm).items()}
    layout.update(
        x0=V((T, D), BF16), x1=V((T, D), BF16), gb1=V((T, D), BF16),
        raw_qkv=V(raw[0], BF16), raw_ot=V(raw[2], BF16), turn2=V(part[2], BF16),
        k=V((T, HP), BF16), vt=V((HP, T), BF16), bias=V((KR, QB), F32), turned=V((HP, T), F32),
        ctab=V((T, LANES), F32), stab=V((T, LANES), F32), small=V((2, 8, W), F32), small_own=rows,
        acc=V((2, 8, W), F32), core_sm=rows, own_sm=rows, dp_sm=V((n_z, 8, W), F32), row_sm=rows,
        all_sm=V((n_t, 8, W), F32),
        gown=V((R, D), F32), gb_own=V((R, D), BF16), yown=V((R, D), F32), x1_own=V((R, D), BF16),
        xo=V((R, D), BF16), eown=V((R, D), F32), ysend=peers, yrecv=peers, esend=peers, erecv=peers,
        du=V((T, FF), BF16), dc=V((T, HP), BF16), dct=V((HP, T), BF16),
        qm=V((NH * QB, HP), BF16), dcm=V((NH * QB, HP), BF16), dctm=V((NH, HP, QB), BF16),
        ds=V((KM, NH * QB), BF16), dk=V((T, HP), F32), dv=V((T, HP), F32), dqkv=V((T, 3 * HP), BF16),
        wg=[V(shape, BF16) for shape in raw],
        pg=[V(shape, BF16) for shape in raw],
        zrecv=[V((n_z - 1, *shape), BF16) for shape in part],
        zsum=[V(shape, F32) for shape in part],
        t_ss=dma((len(CHANNELS), n_t)), t_rs=dma((len(CHANNELS), n_t)),
        w_ss=dma((4, n_z)), w_rs=dma((4, n_z)), f_ss=dma((4, n_z)), f_rs=dma((4, n_z)),
        z_ss=dma((5, n_z)), z_rs=dma((5, n_z)),
        c_ss=dma((8,)), c_rs=dma((8,)),
        lsem=dma((12,)), osem=dma((32,)), isem=dma((40,)),
    )
    return layout


def input_layout():
    return dict(x_hbm=0, cot_hbm=0, raw0=1, raw1=1, raw2=1, raw3=1, seg=1, gain=1, shift=1, qv=1, up=1, resid=1)


SMALL, CORE_SUM, OUT_Y, OUT_G, HAND = range(5)
STAGE_SAVES = (("a", "m", "n", "q", "v", "kt", "wqkv"), ("pt", "c"), ("h", "slope", "wup"), ("wot", "wdt"))
PIECE_WAITS = (("q", "v", "kt", "wqkv", "pt", "c"), ("wup", "h", "slope"), ("wot",), ("wdt",))


def whole_step(dm, trees, *refs):
    r = Refs()
    counts = [tree.num_leaves for tree in trees]
    first = 0
    for tree, count in zip(trees, counts):
        r.__dict__.update(jax.tree.unflatten(tree, refs[first : first + count]))
        first += count
    at = Place(dm)
    s, z, t = at.s, at.z, at.t
    R, T, D, DW = dm.R, dm.T, dm.D, dm.DW
    n_t, n_z = dm.n_t, dm.n_z
    own_rows = rows_of(t, R)
    own_pieces = (r.raw0, r.raw1, r.turn2, r.raw3)
    first_slots = (r.raw_qkv, r.wup, r.raw_ot, r.wdt)
    second_slots = r.land

    def shard(ref, piece, index):
        rows = rows_of(index, DW)
        return ref.at[:, rows, :] if piece == 0 else ref.at[rows, :]

    saves, loads = {}, {}

    def save(src, dst, name):
        copy = pltpu.make_async_copy(src, dst, r.osem.at[len(saves)])
        copy.start()
        saves[name] = copy

    def load(src, dst, name):
        copy = pltpu.make_async_copy(src, dst, r.isem.at[len(loads)])
        copy.start()
        loads[name] = copy

    def to_peer(channel, src, dst, j):
        return remote(src, dst, r.t_ss.at[channel, j], r.t_rs.at[channel, j], TEN, at.tensor_peer(j))

    def spread_block(channel, src, land):
        for j in range(1, n_t):
            to_peer(channel, src, land.at[own_rows, :], j).start()

    def block_arrived(channel, src, land, j):
        to_peer(channel, src, land.at[rows_of(at.tensor_source(j), R), :], j).wait_recv()

    def spread_done(channel, src, land):
        for j in range(1, n_t):
            to_peer(channel, src, land.at[own_rows, :], j).wait_send()

    def to_other_core(channel, src, dst):
        return remote(src, dst, r.c_ss.at[channel], r.c_rs.at[channel], SEC, 1 - s)

    def weight_copy(piece, src, dst, j):
        return remote(src, dst, r.w_ss.at[piece, j], r.w_rs.at[piece, j], DP, at.dp_peer(j))

    def spread(piece, slots):
        for j in range(1, n_z):
            weight_copy(piece, own_pieces[piece], shard(slots[piece], piece, z), j).start()

    def forward_copy(piece, src, dst, index):
        return remote(src, dst, r.f_ss.at[piece, index], r.f_rs.at[piece, index], SEC, 1 - s)

    def pass_on(piece, slots, index, src):
        forward_copy(piece, src, shard(slots[piece], piece, index), index).start()

    def passed_on(piece):
        for j in range(n_z):
            forward_copy(piece, own_pieces[piece], own_pieces[piece], j).wait_send()

    def own_copy(piece, slots):
        return pltpu.make_async_copy(own_pieces[piece], shard(slots[piece], piece, z), r.lsem.at[2 + piece])

    def settle(slots, piece):
        for j in range(1, n_z):
            source = at.dp_source(j)
            landed = shard(slots[piece], piece, source)
            weight_copy(piece, own_pieces[piece], landed, j).wait_recv()
            pass_on(piece, slots, source, landed)
        own_copy(piece, slots).wait()

    def accept(slots, piece):
        for j in range(n_z):
            forward_copy(piece, own_pieces[piece], shard(slots[piece], piece, j), j).wait_recv()

    def ready(slots, layer, piece):
        @pl.when(s == layer)
        def _():
            settle(slots, piece)

        @pl.when(s != layer)
        def _():
            accept(slots, piece)

    def hand_over(piece):
        return to_other_core(HAND + piece, r.wg[piece], r.pg[piece])

    def z_copy(piece, j):
        return remote(
            shard(r.pg[piece], piece, at.dp_peer(j)), r.zrecv[piece].at[j - 1], r.z_ss.at[piece, j],
            r.z_rs.at[piece, j], DP, at.dp_peer(j),
        )

    def merge(piece):
        hand_over(piece).wait_recv()
        total = r.pg[piece][...].astype(F32) + r.wg[piece][...].astype(F32)
        r.pg[piece][...] = total.astype(BF16)
        for j in range(1, n_z):
            z_copy(piece, j).start()

    x_own = r.x_hbm.at[s, 0]
    load(x_own, r.x0.at[own_rows, :], "x0")
    load(r.cot_hbm.at[s, 0], r.gown, "gown")
    pack_small(dm, t, r.gain, r.shift, r.qv, r.up, r.resid, r.small_own)
    at.greet(True)
    spread_block(X0, x_own, r.x0)
    small_copy = to_other_core(SMALL, r.small_own, r.small.at[s])
    small_copy.start()
    load(r.small_own, r.small.at[s], "small")

    @pl.when(s == 0)
    def _():
        for piece in (0, 1):
            spread(piece, first_slots)
            own_copy(piece, first_slots).start()

    turn_shard(dm, r.dqkv, r.raw2, r.turn2)

    @pl.when(s == 0)
    def _():
        for piece in (2, 3):
            spread(piece, first_slots)
            own_copy(piece, first_slots).start()
        for piece in PIECES:
            pass_on(piece, first_slots, z, own_pieces[piece])

    @pl.when(s == 1)
    def _():
        for piece in PIECES:
            own_copy(piece, second_slots).start()

    r.acc[...] = jnp.zeros_like(r.acc)
    loads["gown"].wait()
    r.gb_own[...] = r.gown[...].astype(BF16)
    r.acc[1, 5:6, 0:D] = jnp.sum(r.gown[...], axis=0, keepdims=True)
    loads["small"].wait()
    to_other_core(SMALL, r.small_own, r.small.at[1 - s]).wait_recv()
    gain0, shift0, qvb0, upb0, resid0 = unpack_small(dm, r.small.at[0])
    loads["x0"].wait()
    norm_rows(dm, r.x0, r.a, r.m, r.n, gain0, shift0, t)
    spread_block(GB1, r.gb_own, r.gb1)
    load(r.gb_own, r.gb1.at[own_rows, :], "gb1")
    rotary_tables(dm, r.ctab, r.stab)
    mask_bias(dm, r.seg.at[s], r.bias)
    for j in range(1, n_t):
        block_arrived(X0, x_own, r.x0, j)
        norm_rows(dm, r.x0, r.a, r.m, r.n, gain0, shift0, at.tensor_source(j))

    def forward(params, arrive, after):
        gain, shift, qvb, upb, resid = params
        arrive(0)
        pad_qkv(dm, r.raw_qkv, r.wqkv)

        def project(b, carry):
            project_rows(dm, r.a, r.wqkv, qvb, r.ctab, r.stab, r.q, r.k, r.v, r.dct, r.kt, r.vt, b)
            return carry

        lax.fori_loop(0, T // QB, project, 0)
        after(0)
        attend(dm, r.k, r.dct, r.dctm, r.vt, r.bias, r.pt, r.turned, r.c)
        after(1)
        arrive(1)

        def hidden(b, carry):
            hidden_rows(dm, r.m, r.wup, upb, r.h, r.slope, b)
            return carry

        lax.fori_loop(0, T // QB, hidden, 0)
        after(2)
        arrive(2)
        pad_heads(dm, r.raw_ot, r.wot)
        arrive(3)
        after(3)

    def branches(x_ref, resid, send):
        def body(j, carry):
            r.ysend[j - 1] = branch_rows(dm, r.c, r.h, r.wot, r.wdt, at.tensor_peer(j)).astype(BF16)
            send(j)
            return carry

        lax.fori_loop(1, n_t, body, 0)
        r.yown[...] = (
            branch_rows(dm, r.c, r.h, r.wot, r.wdt, t) + x_ref[own_rows, :].astype(F32) + resid
        )

    def block_copy(channel, src, dst, j):
        return to_peer(channel, src.at[j - 1], dst.at[j - 1], j)

    def sum_blocks(channel, src, dst, total):
        for j in range(1, n_t):
            block_copy(channel, src, dst, j).wait_recv()
            total[...] += dst[j - 1].astype(F32)

    def sends_done(channel, src):
        for j in range(1, n_t):
            block_copy(channel, src, src, j).wait_send()

    def after_first(stage):
        for name in STAGE_SAVES[stage]:
            save(getattr(r, name), r.kept[name], name)

    forward((gain0, shift0, qvb0, upb0, resid0), lambda piece: ready(first_slots, 0, piece), after_first)

    @pl.when(s == 1)
    def _():
        for piece in PIECES:
            spread(piece, second_slots)
        for piece in PIECES:
            pass_on(piece, second_slots, z, own_pieces[piece])

    branches(r.x0, resid0, lambda j: block_copy(Y0, r.ysend, r.yrecv, j).start())
    sum_blocks(Y0, r.ysend, r.yrecv, r.yown)
    r.x1_own[...] = r.yown[...].astype(BF16)
    spread_block(X1, r.x1_own, r.x1)
    load(r.x1_own, r.x1.at[own_rows, :], "x1")

    def local_out(out, own, slot):
        return pltpu.make_async_copy(own, out.at[s], r.lsem.at[slot])

    def place(out, own, layer, channel):
        @pl.when(s == layer)
        def _():
            local_out(out, own, 6 + channel).start()

        @pl.when(s != layer)
        def _():
            to_other_core(channel, own, out.at[s]).start()

    def placed(out, own, layer, channel):
        @pl.when(s == layer)
        def _():
            local_out(out, own, 6 + channel).wait()

        @pl.when(s != layer)
        def _():
            to_other_core(channel, own, out.at[s]).wait_send()

    place(r.o_y, r.yown, 0, OUT_Y)

    gain1, shift1, qvb1, upb1, resid1 = unpack_small(dm, r.small.at[1])
    for name in STAGE_SAVES[0][:3]:
        saves[name].wait()
    loads["x1"].wait()
    norm_rows(dm, r.x1, r.a, r.m, r.n, gain1, shift1, t)
    for j in range(1, n_t):
        block_arrived(X1, r.x1_own, r.x1, j)
        norm_rows(dm, r.x1, r.a, r.m, r.n, gain1, shift1, at.tensor_source(j))

    def arrive_second(piece):
        ready(second_slots, 1, piece)
        for name in PIECE_WAITS[piece]:
            saves[name].wait()

        @pl.when(s == 0)
        def _():
            passed_on(piece)

        copy = pltpu.make_async_copy(second_slots[piece], first_slots[piece], r.isem.at[30 + piece])
        copy.start()
        copy.wait()

    forward((gain1, shift1, qvb1, upb1, resid1), arrive_second, lambda stage: None)
    sends_done(Y0, r.ysend)
    placed(r.o_y, r.yown, 0, OUT_Y)
    branches(r.x1, resid1, lambda j: None)

    def backward(layer, gb_ref, gain, early):
        acc = r.acc.at[layer]
        back_heads(dm, at, gb_ref, r.wot, r.dc, r.dct)
        back_hidden(dm, r, gb_ref, acc)
        early()
        attend_back(
            dm, r.q, r.v, r.kt, r.pt, r.dc, r.dct, r.qm, r.dcm, r.dctm, r.ds, r.dk, r.dv, r.turned
        )
        channel = (E0, E1)[layer]

        def body(j, carry):
            r.esend[j - 1] = back_rows(dm, r, gain, acc, at.tensor_peer(j)).astype(BF16)
            block_copy(channel, r.esend, r.erecv, j).start()
            return carry

        lax.fori_loop(1, n_t, body, 0)
        r.eown[...] = back_rows(dm, r, gain, acc, t)

    for j in range(1, n_t):
        block_arrived(GB1, r.gb_own, r.gb1, j)
    loads["gb1"].wait()
    backward(1, r.gb1, gain1, lambda: None)

    for piece in (3, 1, 0, 2):
        weight_grad(dm, r, piece, r.gb1)

        @pl.when(s == 0)
        def _(piece=piece):
            hand_over(piece).start()

    for name in r.kept:
        load(r.kept[name], getattr(r, name), name)
    load(x_own, r.xo, "xo")

    @pl.when(s == 1)
    def _():
        for piece in (3, 1, 0, 2):
            merge(piece)

    sum_blocks(E1, r.esend, r.erecv, r.eown)
    r.gown[...] += norm_back(r.eown[...], r.x1[own_rows, :].astype(F32))
    spread_done(GB1, r.gb_own, r.gb1)
    r.gb_own[...] = r.gown[...].astype(BF16)
    spread_block(GB0, r.gb_own, r.x0)
    load(r.gb_own, r.x0.at[own_rows, :], "gb0")
    for j in range(1, n_t):
        block_copy(Y1, r.ysend, r.yrecv, j).start()
    place(r.o_g, r.gown, 1, OUT_G)
    r.acc[0, 5:6, 0:D] = jnp.sum(r.gown[...], axis=0, keepdims=True)

    for name in r.kept:
        loads[name].wait()
    loads["gb0"].wait()
    for j in range(1, n_t):
        block_arrived(GB0, r.gb_own, r.x0, j)
    sends_done(E1, r.esend)

    def grad_piece(piece):
        @pl.when(s == 0)
        def _():
            hand_over(piece).wait_send()

        weight_grad(dm, r, piece, r.x0)

        @pl.when(s == 1)
        def _():
            hand_over(piece).start()

    def early():
        for piece in (3, 1, 2):
            grad_piece(piece)

        @pl.when(s == 0)
        def _():
            for piece in (3, 1, 2):
                merge(piece)

    backward(0, r.x0, gain0, early)

    core_copy = to_other_core(CORE_SUM, r.acc.at[1 - s], r.core_sm)
    core_copy.start()
    grad_piece(0)
    core_copy.wait_recv()
    r.own_sm[...] = r.acc[s] + r.core_sm[...]

    def dp_small(j):
        return remote(r.own_sm, r.dp_sm.at[j], r.z_ss.at[4, j], r.z_rs.at[4, j], DP, at.dp_peer(j))

    for j in range(1, n_z):
        dp_small(j).start()

    @pl.when(s == 0)
    def _():
        merge(0)

    sum_blocks(Y1, r.ysend, r.yrecv, r.yown)
    place(r.o_y, r.yown, 1, OUT_Y)
    total = r.own_sm[...]
    for j in range(1, n_z):
        dp_small(j).wait_recv()
        total = total + r.dp_sm[j]
    r.row_sm[...] = total

    def tensor_small(j, slot):
        return to_peer(TS, r.row_sm, r.all_sm.at[slot], j)

    for j in range(1, n_t):
        tensor_small(j, t).start()
    r.all_sm[t] = total

    sum_blocks(E0, r.esend, r.erecv, r.eown)
    placed(r.o_g, r.gown, 1, OUT_G)
    loads["xo"].wait()
    r.gown[...] += norm_back(r.eown[...], r.xo[...].astype(F32))
    place(r.o_g, r.gown, 0, OUT_G)
    for j in range(1, n_t):
        tensor_small(j, at.tensor_source(j)).wait_recv()
    save(r.all_sm, r.o_small, "small")

    for piece in (3, 1, 2, 0):
        kept = r.zsum[piece]
        kept[...] = shard(r.pg[piece], piece, z)[...].astype(F32)
        for j in range(1, n_z):
            z_copy(piece, j).wait_recv()
            kept[...] += r.zrecv[piece][j - 1].astype(F32)
        save(kept, r.o_w[piece], piece)

    for piece in PIECES:
        for j in range(1, n_z):
            z_copy(piece, j).wait_send()
            weight_copy(piece, own_pieces[piece], own_pieces[piece], j).wait_send()

        @pl.when(s == 1)
        def _(piece=piece):
            hand_over(piece).wait_send()
            passed_on(piece)

    small_copy.wait_send()
    core_copy.wait_send()
    for j in range(1, n_z):
        dp_small(j).wait_send()
    for j in range(1, n_t):
        tensor_small(j, t).wait_send()
    spread_done(X0, x_own, r.x0)
    spread_done(X1, r.x1_own, r.x1)
    spread_done(GB0, r.gb_own, r.x0)
    sends_done(Y1, r.ysend)
    sends_done(E0, r.esend)
    placed(r.o_y, r.yown, 1, OUT_Y)
    placed(r.o_g, r.gown, 0, OUT_G)
    to_other_core(OUT_Y, r.yown, r.o_y.at[1 - s]).wait_recv()
    to_other_core(OUT_G, r.gown, r.o_g.at[1 - s]).wait_recv()
    for piece in PIECES:
        saves[piece].wait()
    saves["small"].wait()


def run_step(dm, args):
    kinds = dict(input_layout())
    outs, scratch = out_layout(dm), scratch_layout(dm)
    out_leaves, out_tree = jax.tree.flatten(outs)
    scratch_leaves, scratch_tree = jax.tree.flatten(scratch)
    in_leaves, in_tree = jax.tree.flatten(kinds)
    vmem, anywhere = pl.BlockSpec(memory_space=pltpu.VMEM), pl.BlockSpec(memory_space=ANY)
    made = pl.pallas_call(
        functools.partial(whole_step, dm, (in_tree, out_tree, scratch_tree)),
        out_shape=out_leaves,
        in_specs=[vmem if kind else anywhere for kind in in_leaves],
        out_specs=[anywhere] * len(out_leaves),
        scratch_shapes=scratch_leaves,
        compiler_params=pltpu.CompilerParams(
            collective_id=0, has_side_effects=True, vmem_limit_bytes=VMEM_LIMIT
        ),
        name="whole_step",
    )(*jax.tree.leaves(args))
    return jax.tree.unflatten(out_tree, made)


def write_results(dm, y, g, w0, w1, w2, w3, small, *rest):
    oy, og, oqkv, oout, oup, odown, ogain, oshift, oqv, oupb, oresid = rest[:11]
    by, bg, bqkv, bup, b2, b3, wide, t2, sm, vgain, vshift, vqv, vupb, vresid, isem, osem = rest[11:]
    through = ((y, by, oy), (g, bg, og), (w0, bqkv, oqkv), (w1, bup, oup), (w3, b3, odown))
    into = [pltpu.make_async_copy(src, mid, isem.at[i]) for i, (src, mid, _) in enumerate(through)]
    into += [
        pltpu.make_async_copy(src, dst, isem.at[5 + i]) for i, (src, dst) in enumerate(((small, sm), (w2, b2)))
    ]
    for i in (5, 6, 0, 1, 2, 3, 4):
        into[i].start()
    out = []

    def leave(src, dst):
        copy = pltpu.make_async_copy(src, dst, osem.at[len(out)])
        copy.start()
        out.append(copy)

    into[5].wait()
    total = sm[0]
    for i in range(1, dm.n_t):
        total = total + sm[i]
    vgain[...] = total[0:2, 0 : dm.D]
    vshift[...] = total[2:4, 0 : dm.D]
    vresid[...] = total[5:6, 0 : dm.D]
    vqv[...] = jnp.concatenate([sm[i, 6:8, 0 : dm.HC] for i in range(dm.n_t)], axis=1)
    vupb[...] = jnp.concatenate([sm[i, 4:5, 0 : dm.FF] for i in range(dm.n_t)], axis=1)
    for src, dst in ((vgain, ogain), (vshift, oshift), (vresid, oresid), (vqv, oqv), (vupb, oupb)):
        leave(src, dst)
    into[6].wait()
    turn_shard(dm, wide, b2, t2)
    leave(t2, oout)
    for i, (_, mid, dst) in enumerate(through):
        into[i].wait()
        leave(mid, dst)
    for copy in out:
        copy.wait()


def run_results(dm, made):
    S, V, dma = jax.ShapeDtypeStruct, pltpu.VMEM, pltpu.SemaphoreType.DMA
    block, part = (dm.n_s, dm.R, dm.D), part_shapes(dm)
    turned = (dm.HC, dm.DW)
    pair, wide_up, one = (2, dm.D), (1, dm.n_t * dm.FF), (1, dm.D)
    heads = (2, dm.n_t * dm.HC)
    shapes = [block, block, part[0], turned, part[1], part[3], pair, pair, heads, wide_up, one]
    held = [block, block, part[0], part[1], part[2], part[3], (QB, max(dm.DW, dm.HP)), turned]
    held += [(dm.n_t, 8, small_width(dm)), pair, pair, heads, wide_up, one]
    anywhere = pl.BlockSpec(memory_space=ANY)
    return pl.pallas_call(
        functools.partial(write_results, dm),
        out_shape=[S(shape, F32) for shape in shapes],
        in_specs=[anywhere] * 7,
        out_specs=[anywhere] * 11,
        scratch_shapes=[V(shape, F32) for shape in held] + [dma((7,)), dma((11,))],
        compiler_params=pltpu.CompilerParams(vmem_limit_bytes=VMEM_LIMIT),
        name="write_results",
    )(made["o_y"], made["o_g"], *made["o_w"], made["o_small"])


def body(
    mesh_shape,
    inputs, segment_ids, cotangent, qkv_weight, out_weight, up_weight, down_weight,
    norm_gain, norm_bias, qv_bias, up_bias, resid_bias,
):
    dm = Dims(mesh_shape, inputs.shape, segment_ids.shape, qkv_weight.shape, up_weight.shape)
    made = run_step(
        dm,
        dict(
            x_hbm=inputs, cot_hbm=cotangent, raw0=qkv_weight[0], raw1=up_weight[0], raw2=out_weight[0],
            raw3=down_weight[0].T, seg=segment_ids, gain=norm_gain[0], shift=norm_bias[0], qv=qv_bias[0],
            up=up_bias, resid=resid_bias,
        ),
    )
    y, g, qkv, out, up, down, gain, shift, qv, upb, resid = run_results(dm, made)
    return (
        y[None, :, None], g[None, :, None], qkv[None], out[None], up[None], down.T[None],
        gain[None], shift[None], qv[None], upb, resid,
    )


def solution(mesh):
    rows = P(None, DP, TEN, None)
    both = P(SEC, None, DP, TEN, None)
    weights = (P(SEC, None, DP, TEN), P(SEC, TEN, DP), P(SEC, DP, TEN), P(SEC, TEN, DP))
    vectors = (P(SEC, None, None),) * 3 + (P(SEC, None),) * 2
    return jax.shard_map(
        functools.partial(body, dict(mesh.shape)),
        mesh=mesh,
        in_specs=(rows, P(None, DP, None), rows, *weights, *vectors),
        out_specs=(both, both, *weights, *vectors),
        check_vma=False,
    )
```
